32 devices in a mesh: groups: 2 (over x), steps: 16 (over z, y, core).
Axes of the slice: x: 2, y: 2, z: 4, core: 2. Of those that a mesh axis runs over, the one named last changes fastest.
Arguments:
- states: float32 [32, 4, 4096], P(('groups', 'steps')), parts along dimension 0, may hold values from -6 to 6
- t_sched: int32 [66], P('groups'), parts along dimension 0, may hold values from 0 to 999, as said below
- advances: int32 [4], P('groups'), parts along dimension 0, may hold values from 1 to 16, as said below
- in_weight: bfloat16 [320, 4], replicated, may hold values from -3 to 3
- time_weight: float32 [320, 320], replicated, may hold values from -0.3125 to 0.3125
- mid_weight: bfloat16 [320, 320], replicated, may hold values from -0.3125 to 0.3125
- out_weight: bfloat16 [4, 320], replicated, may hold values from -0.3125 to 0.3125
Outputs:
- final_states: float32 [32, 4, 4096], P(('groups', 'steps')), parts along dimension 0
- errors: float32 [4, 4, 16], P('groups', None, 'steps'), parts along dimension 0
The draws below stay inside these ranges and needn't reach their ends.
There are 2 independent parts, one for each index of `groups`. The reference program is written for one: setup_inputs(seed, part) draws one part's arguments, and reference() takes and returns one part's arrays. A program takes and returns all parts, laid end to end along the dimension named above; an argument that names none is the same for every part. Nothing has to cross between parts.
Inputs may be any that keep to these rules, and one draw needn't show every extreme that they name: `t_sched`: strictly decreasing. Some round advances by exactly 16.
All inputs are finite; a program needn't handle non-finite values.
Results may differ from the reference program's by a relative error of at most 0.0024.
Values sent between devices are 32-bit elements; how exact they have to be, the bound alone decides.
A program may use at most 64 MiB of HBM per device.

```python
import math
import jax
import jax.numpy as jnp
from jax import lax

CH = 320
LAT = 4
TSTEPS = 1000
ROWS = 4096
ITERS = 4
ROUNDS = 2
WINDOW = 16
SCHED = 33
ADV_MOST = 16


def draw_t_sched(key, part):
    picked = jax.random.permutation(key, TSTEPS)[:SCHED].astype(jnp.int32)
    return -jnp.sort(-picked)


def draw_advances(key, part):
    first_key = jax.random.fold_in(key, 11)
    second_key = jax.random.fold_in(key, 12)
    values = jax.random.randint(first_key, (ROUNDS,), 1, ADV_MOST + 1).astype(jnp.int32)
    chosen = jax.random.randint(second_key, (), 0, ROUNDS)
    return jnp.where(jnp.arange(ROUNDS) == chosen, ADV_MOST, values).astype(jnp.int32)


def block_levels(key, dims, shards, low, high):
    loudness = 1.0
    for position, blocks in shards:
        draws = jax.random.uniform(jax.random.fold_in(jax.random.fold_in(key, 6), position), (blocks,), jnp.float32, low / len(shards), high / len(shards))
        loudness = loudness * jnp.repeat(jnp.exp(draws), dims[position] // blocks).reshape((-1,) + (1,) * (len(dims) - 1 - position))
    return loudness


def gaussian(stream_key, shape, width, limit, cuts=(), kind=jnp.bfloat16):
    entries = jax.random.normal(stream_key, shape, jnp.float32) * width
    if len(cuts) > 0:
        entries = block_levels(stream_key, shape, cuts, -0.22, 0.18) * entries
    return jnp.clip(entries, min=-limit, max=limit).astype(kind)


def setup_inputs(seed: int = 0, part: int = 0) -> dict:
    streams_of = jax.random.split(jax.random.key(seed), 8)
    own_keys = jax.random.split(jax.random.fold_in(streams_of[7], part), 8)
    states = gaussian(own_keys[0], (WINDOW, LAT, ROWS), 1.0, 6.0, ((0, 16),), jnp.float32)
    t_sched = draw_t_sched(jax.random.fold_in(jax.random.fold_in(streams_of[7], part), 71), part)
    advances = draw_advances(jax.random.fold_in(jax.random.fold_in(streams_of[7], part), 71), part)
    in_weight = gaussian(streams_of[3], (CH, LAT), LAT ** -0.5, 3.0)
    time_weight = gaussian(streams_of[4], (CH, CH), CH ** -0.5, 0.3125, (), jnp.float32)
    mid_weight = gaussian(streams_of[5], (CH, CH), CH ** -0.5, 0.3125)
    out_weight = gaussian(streams_of[6], (LAT, CH), CH ** -0.5, 0.3125)
    return dict(states=states, t_sched=t_sched, advances=advances, in_weight=in_weight, time_weight=time_weight, mid_weight=mid_weight, out_weight=out_weight)


def alpha_table():
    levels = jnp.arange(TSTEPS, dtype=jnp.float32)
    low = math.sqrt(0.00085)
    high = math.sqrt(0.012)
    betas = (low + (high - low) * levels / (TSTEPS - 1)) ** 2
    return jnp.exp(jnp.cumsum(jnp.log1p(-betas)))

def time_features(stamp):
    halfwidth = CH // 2
    freqs = jnp.exp(-math.log(10000.0) * jnp.arange(halfwidth, dtype=jnp.float32) / halfwidth)
    angles = stamp.astype(jnp.float32) * freqs
    return jnp.concatenate([jnp.cos(angles), jnp.sin(angles)])

def denoise(state, embed, in_weight, mid_weight, out_weight):
    pre = jnp.dot(in_weight, state.astype(jnp.bfloat16), preferred_element_type=jnp.float32) + embed[:, None]
    hidden_one = jax.nn.silu(pre).astype(jnp.bfloat16)
    mixed = jnp.dot(mid_weight, hidden_one, preferred_element_type=jnp.float32)
    hidden_two = (jax.nn.silu(mixed) + pre).astype(jnp.bfloat16)
    return jnp.dot(out_weight, hidden_two, preferred_element_type=jnp.float32)

def reference(states, t_sched, advances, in_weight, time_weight, mid_weight, out_weight):
    alphas = alpha_table()
    window = states.shape[0]
    places = jnp.arange(window, dtype=jnp.int32)
    current = states
    window_start = jnp.int32(0)
    error_rows = []
    for round_no in range(ROUNDS):
        stamp_now = t_sched[window_start + places]
        stamp_next = t_sched[window_start + places + 1]
        alpha_now = alphas[stamp_now]
        alpha_next = alphas[stamp_next]
        coef_one = jnp.sqrt(alpha_next / alpha_now)
        coef_two = jnp.sqrt(1.0 - alpha_next) - coef_one * jnp.sqrt(1.0 - alpha_now)
        feats = jax.vmap(time_features)(stamp_now)
        embeds = jnp.dot(feats, time_weight.T, precision=lax.Precision.HIGHEST)
        sweep_rows = []
        for sweep in range(ITERS):
            noise = lax.map(lambda pair: denoise(pair[0], pair[1], in_weight, mid_weight, out_weight), (current, embeds))
            drift = (coef_one - 1.0)[:, None, None] * current + coef_two[:, None, None] * noise
            totals = jnp.cumsum(drift, axis=0)
            prefix = jnp.concatenate([jnp.zeros_like(drift[:1]), totals[:-1]], axis=0)
            updated = current[0:1] + prefix
            updated = jnp.concatenate([current[0:1], updated[1:]], axis=0)
            sweep_rows.append(lax.optimization_barrier(jnp.mean((updated - current) ** 2, axis=(1, 2))))
            current = updated
        error_rows.append(jnp.stack(sweep_rows))
        advance = advances[round_no]
        source = jnp.minimum(places + advance, window - 1).astype(jnp.int32)
        current = current[source]
        window_start = window_start + advance
    return (current, jnp.stack(error_rows))
```

```python
import functools
import math

import jax
import jax.numpy as jnp
import numpy as np
from jax import lax
from jax.experimental import pallas as pl
from jax.experimental.pallas import tpu as pltpu
from jax.sharding import PartitionSpec as P

TSTEPS = 1000
ITERS = 4
ROUNDS = 2
LANES = 128
BASE = 32
XROWS = 16
GROUP_MOST = 15


def alpha_table():
    levels = np.arange(TSTEPS, dtype=np.float64)
    low = math.sqrt(0.00085)
    high = math.sqrt(0.012)
    betas = (low + (high - low) * levels / (TSTEPS - 1)) ** 2
    return np.exp(np.cumsum(np.log1p(-betas))).astype(np.float32)


def trig_tables(width):
    half = width // 2
    freqs = np.exp(-math.log(10000.0) * np.arange(half, dtype=np.float64) / half)[:, None]
    digits = np.arange(BASE, dtype=np.float64)[None]
    high, low = freqs * digits * BASE, freqs * digits
    coarse = np.concatenate([np.cos(high), np.sin(high)]).astype(np.float32)
    fine = np.concatenate([np.cos(low), np.sin(low)]).astype(np.float32)
    return coarse, fine


def round_up(value, unit):
    return -(-value // unit) * unit


def kernel(
    n, pix, width, depth, group, direct,
    states_ref, sched_ref, adv_ref, alpha_ref, inw_ref, timew_ref, midw_ref, outw_ref, coarse_ref, fine_ref,
    out_ref, err_ref,
    xin, xs, fin, errs, erecv, lhs, mid, outw, coef_one, coef_two, spread,
    in_send, in_recv, out_send, out_recv, err_send, err_recv,
):
    lat = outw_ref.shape[0]
    ch = midw_ref.shape[0]
    me = lax.axis_index("steps")
    span = ROUNDS * n
    f32, bf16 = jnp.float32, jnp.bfloat16

    def peer(hop):
        return lax.rem(me + hop, n)

    def source(d):
        if direct:
            return states_ref.at[0, :, pl.ds(pl.multiple_of(d * pix, LANES), pix)]
        return states_ref.at[d]

    def target(d):
        if direct:
            return out_ref.at[0, :, pl.ds(pl.multiple_of(d * pix, LANES), pix)]
        return out_ref.at[d]

    def in_copy(d, slot):
        return pltpu.make_async_remote_copy(
            src_ref=source(d), dst_ref=xin.at[slot], send_sem=in_send.at[d], recv_sem=in_recv.at[slot],
            device_id={"steps": d}, device_id_type=pl.DeviceIdType.MESH)

    def out_copy(d, slot):
        return pltpu.make_async_remote_copy(
            src_ref=fin.at[d], dst_ref=target(slot), send_sem=out_send.at[d], recv_sem=out_recv.at[slot],
            device_id={"steps": d}, device_id_type=pl.DeviceIdType.MESH)

    def err_copy(d, slot):
        return pltpu.make_async_remote_copy(
            src_ref=errs.at[d], dst_ref=erecv.at[slot], send_sem=err_send.at[d], recv_sem=err_recv.at[slot],
            device_id={"steps": d}, device_id_type=pl.DeviceIdType.MESH)

    def each_peer(act):
        if n <= 16:
            for hop in range(1, n):
                act(peer(hop))
        else:
            @pl.loop(1, n)
            def _(hop):
                act(peer(hop))

    barrier = pltpu.get_barrier_semaphore()
    each_peer(lambda d: pl.semaphore_signal(
        barrier, inc=1, device_id={"steps": d}, device_id_type=pl.DeviceIdType.MESH))

    lane = lax.broadcasted_iota(jnp.int32, (1, depth), 1) - XROWS
    member = jnp.where((lane >= 0) & (lane < 3 * span), lax.rem(jnp.maximum(lane, 0), span), -1)
    advance_one = adv_ref[0]

    def coefficients(m, stamps):
        place = jnp.where(m >= n, advance_one + m - n, m)
        now, after = sched_ref[place], sched_ref[place + 1]
        a_now = jnp.full((8, LANES), alpha_ref[now], f32)
        a_after = jnp.full((8, LANES), alpha_ref[after], f32)
        one = jnp.sqrt(a_after / a_now)
        two = jnp.sqrt(1.0 - a_after) - one * jnp.sqrt(1.0 - a_now)
        coef_one[m] = one - 1.0
        coef_two[m] = two
        return jnp.where(member == m, now, stamps)

    stamps = lax.fori_loop(0, span, coefficients, jnp.zeros((1, depth), jnp.int32), unroll=4)

    pl.semaphore_wait(barrier, n - 1)
    each_peer(lambda d: in_copy(d, me).start())

    digit = lax.broadcasted_iota(jnp.int32, (BASE, depth), 0)
    hot_high = (digit == lax.shift_right_logical(stamps, 5)).astype(f32)
    hot_low = (digit == lax.bitwise_and(stamps, BASE - 1)).astype(f32)
    exact = lax.Precision.HIGHEST
    high = jnp.dot(coarse_ref[...], hot_high, precision=exact, preferred_element_type=f32)
    low = jnp.dot(fine_ref[...], hot_low, precision=exact, preferred_element_type=f32)
    half = ch // 2
    cos_h, sin_h, cos_l, sin_l = high[:half], high[half:], low[:half], low[half:]
    feats = jnp.concatenate([cos_h * cos_l - sin_h * sin_l, sin_h * cos_l + cos_h * sin_l], axis=0)
    embed = 0.5 * jnp.dot(timew_ref[...], feats, precision=exact, preferred_element_type=f32)
    spread[...] = jnp.zeros_like(spread)
    spread[:, 0:lat] = inw_ref[...].astype(f32) * 0.5
    top = embed.astype(bf16).astype(f32)
    rest = embed - top
    middle = rest.astype(bf16).astype(f32)
    bottom = (rest - middle).astype(bf16).astype(f32)
    part = jnp.where(lane < span, top, jnp.where(lane < 2 * span, middle, bottom))
    part = jnp.where(member >= 0, part, 0.0)
    lhs[...] = (spread[...] + part).astype(bf16)
    mid[...] = (midw_ref[...].astype(f32) * 0.5).astype(bf16)
    outw[...] = jnp.zeros_like(outw)
    outw[0:lat, :] = outw_ref[...].astype(f32)

    xs[...] = jnp.zeros_like(xs)
    if direct:
        xs[me, 0:lat, :] = states_ref[0, :, pl.ds(pl.multiple_of(me * pix, LANES), pix)]
    else:
        xs[me, 0:lat, :] = states_ref[me]

    def arrived(d):
        in_copy(d, d).wait_recv()
        xs[d, 0:lat, :] = xin[d]

    each_peer(arrived)

    hot_row = lax.broadcasted_iota(jnp.int32, (depth - XROWS, LANES), 0)
    hot_member = jnp.where(hot_row < 3 * span, lax.rem(hot_row, span), -1)
    outs = outw[...].astype(bf16)
    wide = lambda tile: jnp.concatenate([tile] * (width // LANES), axis=1) if width > LANES else tile

    def first(x, m):
        hot = wide((hot_member == m).astype(f32).astype(bf16))
        padded = jnp.concatenate([x, jnp.zeros((XROWS - 8, width), f32)], axis=0).astype(bf16)
        pre = jnp.dot(lhs[...], jnp.concatenate([padded, hot], axis=0), preferred_element_type=f32)
        return pre, (pre + pre * jnp.tanh(pre)).astype(bf16)

    def second(pre, hidden):
        mixed = jnp.dot(mid[...], hidden, preferred_element_type=f32)
        return (mixed * (1.0 + jnp.tanh(mixed)) + (pre + pre)).astype(bf16)

    def third(hidden):
        return jnp.dot(outs, hidden, preferred_element_type=f32)

    def note_error(row, k, change):
        square = change * change
        if pix < width:
            square = jnp.where(lax.broadcasted_iota(jnp.int32, square.shape, 1) < pix, square, 0.0)
        total = square[:, 0:LANES]
        for start in range(LANES, width, LANES):
            total = total + square[:, start:start + LANES]
        errs[k, pl.ds(row, 1), :] = jnp.sum(total, axis=0, keepdims=True)

    def one_round(r, carry):
        def sweep(i, carry):
            row = r * ITERS + i

            def some(g, running):
                ks = [g * group + j for j in range(group)]
                olds = [xs[k] for k in ks]
                ones = [None] * group
                twos = [None] * group
                noises = [None] * group
                for step in range(group + 2):
                    if step < group:
                        ones[step] = first(olds[step], r * n + ks[step])
                    if 0 <= step - 1 < group:
                        twos[step - 1] = second(*ones[step - 1])
                    if 0 <= step - 2 < group:
                        noises[step - 2] = third(twos[step - 2])
                for j, k in enumerate(ks):
                    m = r * n + k
                    note_error(row, k, running - olds[j])
                    xs[k] = running
                    running = running + (wide(coef_one[m]) * olds[j] + wide(coef_two[m]) * noises[j])
                return running

            running = lax.fori_loop(0, (n - 1) // group, some, xs[0])
            note_error(row, n - 1, running - xs[n - 1])
            xs[n - 1] = running
            return carry

        lax.fori_loop(0, ITERS, sweep, 0)
        advance = adv_ref[r]

        def shift(k, carry):
            xs[k] = xs[jnp.minimum(k + advance, n - 1)]
            return carry

        lax.fori_loop(0, n, shift, 0, unroll=4)
        return carry

    lax.fori_loop(0, ROUNDS, one_round, 0)
    for k in range(n):
        fin[k] = xs[k, 0:lat, :]
    each_peer(lambda d: out_copy(d, me).start())
    each_peer(lambda d: err_copy(d, me).start())
    if direct:
        out_ref[0, :, pl.ds(pl.multiple_of(me * pix, LANES), pix)] = fin[me]
    else:
        out_ref[me] = fin[me]
    erecv[me] = errs[me]
    each_peer(lambda d: err_copy(d, d).wait_recv())
    sums = lax.fori_loop(0, n, lambda k, total: total + erecv[k], jnp.zeros((ROUNDS * ITERS, LANES), f32), unroll=4)
    err_ref[...] = jnp.sum(sums, axis=1, keepdims=True) * (1.0 / (lat * n * pix))
    each_peer(lambda d: out_copy(d, d).wait_recv())
    each_peer(lambda d: in_copy(d, me).wait_send())
    each_peer(lambda d: out_copy(d, me).wait_send())
    each_peer(lambda d: err_copy(d, me).wait_send())


def shards(states, t_sched, advances, in_weight, time_weight, mid_weight, out_weight):
    n = lax.axis_size("steps")
    _, lat, rows = states.shape
    ch = mid_weight.shape[0]
    pix = rows // n
    direct = pix % LANES == 0
    width = round_up(pix, LANES)
    depth = round_up(XROWS + 3 * ROUNDS * n, LANES)
    group = max(g for g in range(1, GROUP_MOST + 1) if (n - 1) % g == 0)
    coarse, fine = trig_tables(time_weight.shape[1])
    if direct:
        sent = states
        out_shape = states.shape
    else:
        sent = jnp.pad(states.reshape(lat, n, pix).transpose(1, 0, 2), ((0, 0), (0, 0), (0, width - pix)))
        out_shape = sent.shape
    vmem = pl.BlockSpec(memory_space=pltpu.VMEM)
    smem = pl.BlockSpec(memory_space=pltpu.SMEM)
    f32, bf16 = jnp.float32, jnp.bfloat16
    final, errors = pl.pallas_call(
        functools.partial(kernel, n, pix, width, depth, group, direct),
        out_shape=(jax.ShapeDtypeStruct(out_shape, f32), jax.ShapeDtypeStruct((ROUNDS * ITERS, 1), f32)),
        in_specs=[vmem, smem, smem, smem, vmem, vmem, vmem, vmem, vmem, vmem],
        out_specs=(vmem, vmem),
        scratch_shapes=[
            pltpu.VMEM((n, lat, width), f32),
            pltpu.VMEM((n, 8, width), f32),
            pltpu.VMEM((n, lat, width), f32),
            pltpu.VMEM((n, ROUNDS * ITERS, LANES), f32),
            pltpu.VMEM((n, ROUNDS * ITERS, LANES), f32),
            pltpu.VMEM((ch, depth), bf16),
            pltpu.VMEM((ch, ch), bf16),
            pltpu.VMEM((8, ch), f32),
            pltpu.VMEM((ROUNDS * n, 8, LANES), f32),
            pltpu.VMEM((ROUNDS * n, 8, LANES), f32),
            pltpu.VMEM((ch, depth), f32),
        ] + [pltpu.SemaphoreType.DMA((n,))] * 6,
        compiler_params=pltpu.CompilerParams(
            collective_id=0, has_side_effects=True, vmem_limit_bytes=48 * 1024 * 1024),
        name="picard",
    )(sent, t_sched, advances, jnp.asarray(alpha_table()), in_weight, time_weight, mid_weight, out_weight,
      jnp.asarray(coarse), jnp.asarray(fine))
    if not direct:
        final = final[:, :, :pix].transpose(1, 0, 2).reshape(states.shape)
    return final, errors.reshape(ROUNDS, ITERS, 1)


def solution(mesh):
    in_specs = (P(("groups", "steps"), None, None), P("groups"), P("groups"), P(), P(), P(), P())
    out_specs = (P(("groups", "steps"), None, None), P("groups", None, "steps"))
    return jax.shard_map(shards, mesh=mesh, in_specs=in_specs, out_specs=out_specs, check_vma=False)
```

```python
import functools
import math

import jax
import jax.numpy as jnp
import numpy as np
from jax import lax
from jax.experimental import pallas as pl
from jax.experimental.pallas import tpu as pltpu
from jax.sharding import PartitionSpec as P

TSTEPS = 1000
ITERS = 4
ROUNDS = 2
LANES = 128
BASE = 32
XROWS = 16
GROUP_MOST = 15


def alpha_table():
    levels = np.arange(TSTEPS, dtype=np.float64)
    low = math.sqrt(0.00085)
    high = math.sqrt(0.012)
    betas = (low + (high - low) * levels / (TSTEPS - 1)) ** 2
    return np.exp(np.cumsum(np.log1p(-betas))).astype(np.float32)


def trig_tables(width):
    half = width // 2
    freqs = np.exp(-math.log(10000.0) * np.arange(half, dtype=np.float64) / half)[:, None]
    digits = np.arange(BASE, dtype=np.float64)[None]
    high, low = freqs * digits * BASE, freqs * digits
    coarse = np.concatenate([np.cos(high), np.sin(high)]).astype(np.float32)
    fine = np.concatenate([np.cos(low), np.sin(low)]).astype(np.float32)
    return np.concatenate([coarse, fine])


def round_up(value, unit):
    return -(-value // unit) * unit


def kernel(
    n, pix, width, depth, group, direct,
    states_hbm, sched_ref, adv_ref, alpha_ref, inw_hbm, outw_hbm, timew_hbm, midw_hbm, trig_hbm,
    out_ref, err_ref,
    states_ref, inw_ref, outw_ref, timew, midw, trig, xin, xs, fin, errs, elines, erecv, lhs, mid, outw, inw, coef_one, coef_two,
    local, in_send, in_recv, out_send, out_recv, err_send, err_recv,
):
    lat = outw_ref.shape[0]
    ch = midw.shape[0]
    me = lax.axis_index("steps")
    span = ROUNDS * n
    f32, bf16 = jnp.float32, jnp.bfloat16

    def peer(hop):
        return lax.rem(me + hop, n)

    def source(d):
        if direct:
            return states_ref.at[0, :, pl.ds(pl.multiple_of(d * pix, LANES), pix)]
        return states_ref.at[d]

    def target(d):
        if direct:
            return out_ref.at[0, :, pl.ds(pl.multiple_of(d * pix, LANES), pix)]
        return out_ref.at[d]

    def in_copy(d, slot):
        return pltpu.make_async_remote_copy(
            src_ref=source(d), dst_ref=xin.at[slot], send_sem=in_send.at[d], recv_sem=in_recv.at[slot],
            device_id={"steps": d}, device_id_type=pl.DeviceIdType.MESH)

    def out_copy(d, slot):
        return pltpu.make_async_remote_copy(
            src_ref=fin.at[d], dst_ref=target(slot), send_sem=out_send.at[d], recv_sem=out_recv.at[slot],
            device_id={"steps": d}, device_id_type=pl.DeviceIdType.MESH)

    def err_copy(d, slot):
        return pltpu.make_async_remote_copy(
            src_ref=elines.at[d], dst_ref=erecv.at[slot], send_sem=err_send.at[d], recv_sem=err_recv.at[slot],
            device_id={"steps": d}, device_id_type=pl.DeviceIdType.MESH)

    def each_peer(act):
        if n <= 16:
            for hop in range(1, n):
                act(peer(hop))
        else:
            @pl.loop(1, n)
            def _(hop):
                act(peer(hop))

    loads = [
        pltpu.make_async_copy(source_ref, held, local.at[j])
        for j, (source_ref, held) in enumerate((
            (states_hbm, states_ref), (trig_hbm, trig), (timew_hbm, timew), (midw_hbm, midw),
            (inw_hbm, inw_ref), (outw_hbm, outw_ref)))
    ]
    for load in loads:
        load.start()
    barrier = pltpu.get_barrier_semaphore()
    each_peer(lambda d: pl.semaphore_signal(
        barrier, inc=1, device_id={"steps": d}, device_id_type=pl.DeviceIdType.MESH))

    lane = lax.broadcasted_iota(jnp.int32, (1, depth), 1) - XROWS
    member = jnp.where((lane >= 0) & (lane < 3 * span), lax.rem(jnp.maximum(lane, 0), span), -1)
    advance_one = adv_ref[0]

    def coefficients(m, stamps):
        place = jnp.where(m >= n, advance_one + m - n, m)
        now, after = sched_ref[place], sched_ref[place + 1]
        a_now = jnp.full((8, LANES), alpha_ref[now], f32)
        a_after = jnp.full((8, LANES), alpha_ref[after], f32)
        one = jnp.sqrt(a_after / a_now)
        two = jnp.sqrt(1.0 - a_after) - one * jnp.sqrt(1.0 - a_now)
        coef_one[m] = one - 1.0
        coef_two[m] = two
        return jnp.where(member == m, now, stamps)

    stamps = lax.fori_loop(0, span, coefficients, jnp.zeros((1, depth), jnp.int32), unroll=4)

    loads[0].wait()
    pl.semaphore_wait(barrier, n - 1)
    each_peer(lambda d: in_copy(d, me).start())

    digit = lax.broadcasted_iota(jnp.int32, (BASE, depth), 0)
    hot_high = (digit == lax.shift_right_logical(stamps, 5)).astype(f32)
    hot_low = (digit == lax.bitwise_and(stamps, BASE - 1)).astype(f32)
    exact = lax.Precision.HIGHEST
    for load in loads[1:]:
        load.wait()
    high = jnp.dot(trig[0:ch], hot_high, precision=exact, preferred_element_type=f32)
    low = jnp.dot(trig[ch:], hot_low, precision=exact, preferred_element_type=f32)
    half = ch // 2
    cos_h, sin_h, cos_l, sin_l = high[:half], high[half:], low[:half], low[half:]
    feats = jnp.concatenate([cos_h * cos_l - sin_h * sin_l, sin_h * cos_l + cos_h * sin_l], axis=0)
    embed = 0.5 * jnp.dot(timew[...], feats, precision=exact, preferred_element_type=f32)
    inw[...] = jnp.zeros_like(inw)
    inw[0:lat, :] = inw_ref[...].astype(f32) * 0.5
    unit = (lax.broadcasted_iota(jnp.int32, (8, depth), 0) == lane + XROWS).astype(f32)
    spread = lax.dot_general(
        inw[...], unit, (((0,), (0,)), ((), ())), precision=exact, preferred_element_type=f32)
    top = embed.astype(bf16).astype(f32)
    rest = embed - top
    middle = rest.astype(bf16).astype(f32)
    bottom = (rest - middle).astype(bf16).astype(f32)
    part = jnp.where(lane < span, top, jnp.where(lane < 2 * span, middle, bottom))
    part = jnp.where(member >= 0, part, 0.0)
    left = spread + part
    lhs[0:ch, :] = left.astype(bf16)
    mid[...] = (midw[...].astype(f32) * 0.5).astype(bf16)
    outw[...] = jnp.zeros_like(outw)
    outw[0:lat, :] = outw_ref[...].astype(f32)
    linear = 2.0 * jnp.dot(outw[...], left, precision=exact, preferred_element_type=f32)
    linear_top = linear.astype(bf16).astype(f32)
    linear_rest = linear - linear_top
    linear_middle = linear_rest.astype(bf16).astype(f32)
    linear_bottom = linear_rest - linear_middle
    lhs[ch:ch + 32, :] = jnp.concatenate(
        [linear_top, linear_middle, linear_bottom, jnp.zeros_like(linear)], axis=0).astype(bf16)

    xs[...] = jnp.zeros_like(xs)
    if direct:
        xs[me, 0:lat, :] = states_ref[0, :, pl.ds(pl.multiple_of(me * pix, LANES), pix)]
    else:
        xs[me, 0:lat, :] = states_ref[me]

    def arrived(d):
        in_copy(d, d).wait_recv()
        xs[d, 0:lat, :] = xin[d]

    each_peer(arrived)

    hot_row = lax.broadcasted_iota(jnp.int32, (depth - XROWS, LANES), 0)
    hot_member = jnp.where(hot_row < 3 * span, lax.rem(hot_row, span), -1)
    outs = outw[...].astype(bf16)
    wide = lambda tile: jnp.concatenate([tile] * (width // LANES), axis=1) if width > LANES else tile

    def first(x, m):
        hot = wide((hot_member == m).astype(f32).astype(bf16))
        padded = jnp.concatenate([x, jnp.zeros((XROWS - 8, width), f32)], axis=0).astype(bf16)
        both = jnp.dot(lhs[...], jnp.concatenate([padded, hot], axis=0), preferred_element_type=f32)
        pre = both[0:ch]
        tail = both[ch:ch + 8] + both[ch + 8:ch + 16] + both[ch + 16:ch + 24]
        return tail, (pre + pre * jnp.tanh(pre)).astype(bf16)

    def second(tail, hidden):
        mixed = jnp.dot(mid[...], hidden, preferred_element_type=f32)
        return tail, (mixed + mixed * jnp.tanh(mixed)).astype(bf16)

    def third(tail, hidden):
        return tail + jnp.dot(outs, hidden, preferred_element_type=f32)

    def note_error(row, k, change):
        square = change * change
        if pix < width:
            square = jnp.where(lax.broadcasted_iota(jnp.int32, square.shape, 1) < pix, square, 0.0)
        total = square[:, 0:LANES]
        for start in range(LANES, width, LANES):
            total = total + square[:, start:start + LANES]
        errs[k, pl.ds(row, 1), :] = jnp.sum(total, axis=0, keepdims=True)

    def one_round(r, carry):
        def sweep(i, carry):
            row = r * ITERS + i

            def some(g, running):
                ks = [g * group + j for j in range(group)]
                olds = [xs[k] for k in ks]
                ones = [None] * group
                twos = [None] * group
                noises = [None] * group
                for step in range(group + 2):
                    if step < group:
                        ones[step] = first(olds[step], r * n + ks[step])
                    if 0 <= step - 1 < group:
                        twos[step - 1] = second(*ones[step - 1])
                    if 0 <= step - 2 < group:
                        noises[step - 2] = third(*twos[step - 2])
                for j, k in enumerate(ks):
                    m = r * n + k
                    note_error(row, k, running - olds[j])
                    xs[k] = running
                    running = running + (wide(coef_one[m]) * olds[j] + wide(coef_two[m]) * noises[j])
                return running

            running = lax.fori_loop(0, (n - 1) // group, some, xs[0])
            note_error(row, n - 1, running - xs[n - 1])
            xs[n - 1] = running
            return carry

        lax.fori_loop(0, ITERS, sweep, 0)
        advance = adv_ref[r]

        def shift(k, carry):
            xs[k] = xs[jnp.minimum(k + advance, n - 1)]
            return carry

        lax.fori_loop(0, n, shift, 0, unroll=4)
        return carry

    lax.fori_loop(0, ROUNDS, one_round, 0)
    for k in range(n):
        fin[k] = xs[k, 0:lat, :]
    each_peer(lambda d: out_copy(d, me).start())
    cells = (ROUNDS * ITERS, LANES)
    diagonal = lax.broadcasted_iota(jnp.int32, cells, 0) == lax.broadcasted_iota(jnp.int32, cells, 1)
    for k in range(n):
        total = jnp.sum(errs[k], axis=1, keepdims=True)
        elines[k] = jnp.sum(jnp.where(diagonal, total, 0.0), axis=0, keepdims=True)
    each_peer(lambda d: err_copy(d, me).start())
    if direct:
        out_ref[0, :, pl.ds(pl.multiple_of(me * pix, LANES), pix)] = fin[me]
    else:
        out_ref[me] = fin[me]
    erecv[me] = elines[me]
    each_peer(lambda d: err_copy(d, d).wait_recv())
    sums = lax.fori_loop(0, n, lambda k, total: total + erecv[k], jnp.zeros((1, LANES), f32), unroll=4)
    means = jnp.sum(jnp.where(diagonal, sums, 0.0), axis=1, keepdims=True) * (1.0 / (lat * n * pix))
    for r in range(ROUNDS):
        err_ref[r] = means[r * ITERS:(r + 1) * ITERS]
    each_peer(lambda d: out_copy(d, d).wait_recv())
    each_peer(lambda d: in_copy(d, me).wait_send())
    each_peer(lambda d: out_copy(d, me).wait_send())
    each_peer(lambda d: err_copy(d, me).wait_send())


def shards(states, t_sched, advances, in_weight, time_weight, mid_weight, out_weight):
    n = lax.axis_size("steps")
    _, lat, rows = states.shape
    ch = mid_weight.shape[0]
    pix = rows // n
    direct = pix % LANES == 0
    width = round_up(pix, LANES)
    depth = round_up(XROWS + 3 * ROUNDS * n, LANES)
    group = max(g for g in range(1, GROUP_MOST + 1) if (n - 1) % g == 0)
    if direct:
        sent = states
        out_shape = states.shape
    else:
        sent = jnp.pad(states.reshape(lat, n, pix).transpose(1, 0, 2), ((0, 0), (0, 0), (0, width - pix)))
        out_shape = sent.shape
    vmem = pl.BlockSpec(memory_space=pltpu.VMEM)
    smem = pl.BlockSpec(memory_space=pltpu.SMEM)
    hbm = pl.BlockSpec(memory_space=pltpu.HBM)
    f32, bf16 = jnp.float32, jnp.bfloat16
    final, errors = pl.pallas_call(
        functools.partial(kernel, n, pix, width, depth, group, direct),
        out_shape=(jax.ShapeDtypeStruct(out_shape, f32), jax.ShapeDtypeStruct((ROUNDS, ITERS, 1), f32)),
        in_specs=[hbm, smem, smem, smem, hbm, hbm, hbm, hbm, hbm],
        out_specs=(vmem, vmem),
        scratch_shapes=[
            pltpu.VMEM(sent.shape, f32),
            pltpu.VMEM((lat, ch), bf16),
            pltpu.VMEM((lat, ch), bf16),
            pltpu.VMEM((ch, ch), f32),
            pltpu.VMEM((ch, ch), bf16),
            pltpu.VMEM((2 * ch, BASE), f32),
            pltpu.VMEM((n, lat, width), f32),
            pltpu.VMEM((n, 8, width), f32),
            pltpu.VMEM((n, lat, width), f32),
            pltpu.VMEM((n, ROUNDS * ITERS, LANES), f32),
            pltpu.VMEM((n, 1, LANES), f32),
            pltpu.VMEM((n, 1, LANES), f32),
            pltpu.VMEM((ch + 32, depth), bf16),
            pltpu.VMEM((ch, ch), bf16),
            pltpu.VMEM((8, ch), f32),
            pltpu.VMEM((8, ch), f32),
            pltpu.VMEM((ROUNDS * n, 8, LANES), f32),
            pltpu.VMEM((ROUNDS * n, 8, LANES), f32),
            pltpu.SemaphoreType.DMA((6,)),
        ] + [pltpu.SemaphoreType.DMA((n,))] * 6,
        compiler_params=pltpu.CompilerParams(
            collective_id=0, has_side_effects=True, vmem_limit_bytes=67043328),
        name="picard",
    )(sent, t_sched, advances, jnp.asarray(alpha_table()), in_weight.T, out_weight, time_weight, mid_weight,
      jnp.asarray(trig_tables(time_weight.shape[1])))
    if not direct:
        final = final[:, :, :pix].transpose(1, 0, 2).reshape(states.shape)
    return final, errors


def solution(mesh):
    in_specs = (P(("groups", "steps"), None, None), P("groups"), P("groups"), P(), P(), P(), P())
    out_specs = (P(("groups", "steps"), None, None), P("groups", None, "steps"))
    return jax.shard_map(shards, mesh=mesh, in_specs=in_specs, out_specs=out_specs, check_vma=False)
```

```python
import functools
import math

import jax
import jax.numpy as jnp
import numpy as np
from jax import lax
from jax.experimental import pallas as pl
from jax.experimental.pallas import tpu as pltpu
from jax.sharding import PartitionSpec as P

TSTEPS = 1000
ITERS = 4
ROUNDS = 2
LANES = 128
BASE = 32
XROWS = 16
GROUP_MOST = 15


def alpha_table():
    levels = np.arange(TSTEPS, dtype=np.float64)
    low = math.sqrt(0.00085)
    high = math.sqrt(0.012)
    betas = (low + (high - low) * levels / (TSTEPS - 1)) ** 2
    return np.exp(np.cumsum(np.log1p(-betas))).astype(np.float32)


def trig_tables(width):
    half = width // 2
    freqs = np.exp(-math.log(10000.0) * np.arange(half, dtype=np.float64) / half)[:, None]
    digits = np.arange(BASE, dtype=np.float64)[None]
    high, low = freqs * digits * BASE, freqs * digits
    coarse = np.concatenate([np.cos(high), np.sin(high)]).astype(np.float32)
    fine = np.concatenate([np.cos(low), np.sin(low)]).astype(np.float32)
    return np.concatenate([coarse, fine])


def round_up(value, unit):
    return -(-value // unit) * unit


def kernel(
    n, pix, width, depth, direct,
    states_hbm, sched_ref, adv_ref, alpha_ref, inw_hbm, outw_hbm, timew_hbm, midw_hbm, trig_hbm,
    out_ref, err_ref,
    states_ref, inw_ref, outw_ref, timew, midw, trig, xin, xs, fin, errs, elines, erecv, lhs, mid, outw, inw, coef_one, coef_two,
    local, in_send, in_recv, out_send, out_recv, err_send, err_recv,
):
    lat = outw_ref.shape[0]
    ch = midw.shape[0]
    me = lax.axis_index("steps")
    span = ROUNDS * n
    f32, bf16 = jnp.float32, jnp.bfloat16

    def peer(hop):
        return lax.rem(me + hop, n)

    def source(d):
        if direct:
            return states_ref.at[0, :, pl.ds(pl.multiple_of(d * pix, LANES), pix)]
        return states_ref.at[d]

    def target(d):
        if direct:
            return out_ref.at[0, :, pl.ds(pl.multiple_of(d * pix, LANES), pix)]
        return out_ref.at[d]

    def in_copy(d, slot):
        return pltpu.make_async_remote_copy(
            src_ref=source(d), dst_ref=xin.at[slot], send_sem=in_send.at[d], recv_sem=in_recv.at[slot],
            device_id={"steps": d}, device_id_type=pl.DeviceIdType.MESH)

    def out_copy(d, slot):
        return pltpu.make_async_remote_copy(
            src_ref=fin.at[d], dst_ref=target(slot), send_sem=out_send.at[d], recv_sem=out_recv.at[slot],
            device_id={"steps": d}, device_id_type=pl.DeviceIdType.MESH)

    def err_copy(d, slot):
        return pltpu.make_async_remote_copy(
            src_ref=elines.at[d], dst_ref=erecv.at[slot], send_sem=err_send.at[d], recv_sem=err_recv.at[slot],
            device_id={"steps": d}, device_id_type=pl.DeviceIdType.MESH)

    def each_peer(act):
        if n <= 16:
            for hop in range(1, n):
                act(peer(hop))
        else:
            @pl.loop(1, n)
            def _(hop):
                act(peer(hop))

    loads = [
        pltpu.make_async_copy(source_ref, held, local.at[j])
        for j, (source_ref, held) in enumerate((
            (states_hbm, states_ref), (trig_hbm, trig), (timew_hbm, timew), (midw_hbm, midw),
            (inw_hbm, inw_ref), (outw_hbm, outw_ref)))
    ]
    for load in loads:
        load.start()
    barrier = pltpu.get_barrier_semaphore()
    each_peer(lambda d: pl.semaphore_signal(
        barrier, inc=1, device_id={"steps": d}, device_id_type=pl.DeviceIdType.MESH))

    lane = lax.broadcasted_iota(jnp.int32, (1, depth), 1) - XROWS
    member = jnp.where((lane >= 0) & (lane < 3 * span), lax.rem(jnp.maximum(lane, 0), span), -1)
    advance_one = adv_ref[0]

    def coefficients(m, stamps):
        place = jnp.where(m >= n, advance_one + m - n, m)
        now, after = sched_ref[place], sched_ref[place + 1]
        a_now = jnp.full((8, LANES), alpha_ref[now], f32)
        a_after = jnp.full((8, LANES), alpha_ref[after], f32)
        one = jnp.sqrt(a_after / a_now)
        two = jnp.sqrt(1.0 - a_after) - one * jnp.sqrt(1.0 - a_now)
        coef_one[m] = one - 1.0
        coef_two[m] = two
        return jnp.where(member == m, now, stamps)

    stamps = lax.fori_loop(0, span, coefficients, jnp.zeros((1, depth), jnp.int32), unroll=4)

    loads[0].wait()
    pl.semaphore_wait(barrier, n - 1)
    each_peer(lambda d: in_copy(d, me).start())

    digit = lax.broadcasted_iota(jnp.int32, (BASE, depth), 0)
    hot_high = (digit == lax.shift_right_logical(stamps, 5)).astype(f32)
    hot_low = (digit == lax.bitwise_and(stamps, BASE - 1)).astype(f32)
    exact = lax.Precision.HIGHEST
    for load in loads[1:]:
        load.wait()
    high = jnp.dot(trig[0:ch], hot_high, precision=exact, preferred_element_type=f32)
    low = jnp.dot(trig[ch:], hot_low, precision=exact, preferred_element_type=f32)
    half = ch // 2
    cos_h, sin_h, cos_l, sin_l = high[:half], high[half:], low[:half], low[half:]
    feats = jnp.concatenate([cos_h * cos_l - sin_h * sin_l, sin_h * cos_l + cos_h * sin_l], axis=0)
    embed = 0.5 * jnp.dot(timew[...], feats, precision=exact, preferred_element_type=f32)
    inw[...] = jnp.zeros_like(inw)
    inw[0:lat, :] = inw_ref[...].astype(f32) * 0.5
    unit = (lax.broadcasted_iota(jnp.int32, (8, depth), 0) == lane + XROWS).astype(f32)
    spread = lax.dot_general(
        inw[...], unit, (((0,), (0,)), ((), ())), precision=exact, preferred_element_type=f32)
    top = embed.astype(bf16).astype(f32)
    rest = embed - top
    middle = rest.astype(bf16).astype(f32)
    bottom = (rest - middle).astype(bf16).astype(f32)
    part = jnp.where(lane < span, top, jnp.where(lane < 2 * span, middle, bottom))
    part = jnp.where(member >= 0, part, 0.0)
    left = spread + part
    lhs[0:ch, :] = left.astype(bf16)
    mid[...] = (midw[...].astype(f32) * 0.5).astype(bf16)
    outw[...] = jnp.zeros_like(outw)
    outw[0:lat, :] = outw_ref[...].astype(f32)
    linear = 2.0 * jnp.dot(outw[...], left, precision=exact, preferred_element_type=f32)
    linear_top = linear.astype(bf16).astype(f32)
    linear_rest = linear - linear_top
    linear_middle = linear_rest.astype(bf16).astype(f32)
    linear_bottom = linear_rest - linear_middle
    lhs[ch:ch + 32, :] = jnp.concatenate(
        [linear_top, linear_middle, linear_bottom, jnp.zeros_like(linear)], axis=0).astype(bf16)

    xs[...] = jnp.zeros_like(xs)
    errs[...] = jnp.zeros_like(errs)
    if direct:
        xs[me, 0:lat, :] = states_ref[0, :, pl.ds(pl.multiple_of(me * pix, LANES), pix)]
    else:
        xs[me, 0:lat, :] = states_ref[me]

    def arrived(d):
        in_copy(d, d).wait_recv()
        xs[d, 0:lat, :] = xin[d]

    each_peer(arrived)

    hot_row = lax.broadcasted_iota(jnp.int32, (depth - XROWS, LANES), 0)
    hot_member = jnp.where(hot_row < 3 * span, lax.rem(hot_row, span), -1)
    outs = outw[...].astype(bf16)
    wide = lambda tile: jnp.concatenate([tile] * (width // LANES), axis=1) if width > LANES else tile

    def first(x, m):
        hot = wide((hot_member == m).astype(f32).astype(bf16))
        padded = jnp.concatenate([x, jnp.zeros((XROWS - 8, width), f32)], axis=0).astype(bf16)
        both = jnp.dot(lhs[...], jnp.concatenate([padded, hot], axis=0), preferred_element_type=f32)
        pre = both[0:ch]
        tail = both[ch:ch + 8] + both[ch + 8:ch + 16] + both[ch + 16:ch + 24]
        return tail, (pre + pre * jnp.tanh(pre)).astype(bf16)

    def second(tail, hidden):
        mixed = jnp.dot(mid[...], hidden, preferred_element_type=f32)
        return tail, (mixed + mixed * jnp.tanh(mixed)).astype(bf16)

    def third(tail, hidden):
        return tail + jnp.dot(outs, hidden, preferred_element_type=f32)

    def note_error(row, k, change):
        square = change * change
        if pix < width:
            square = jnp.where(lax.broadcasted_iota(jnp.int32, square.shape, 1) < pix, square, 0.0)
        total = square[:, 0:LANES]
        for start in range(LANES, width, LANES):
            total = total + square[:, start:start + LANES]
        errs[k, pl.ds(row, 1), :] = jnp.sum(total, axis=0, keepdims=True)

    def one_round(r, carry):
        def some(row, ks, running):
            count = len(ks)
            olds = [xs[k] for k in ks]
            ones = [None] * count
            twos = [None] * count
            noises = [None] * count
            for step in range(count + 2):
                if step < count:
                    ones[step] = first(olds[step], r * n + ks[step])
                if 0 <= step - 1 < count:
                    twos[step - 1] = second(*ones[step - 1])
                if 0 <= step - 2 < count:
                    noises[step - 2] = third(*twos[step - 2])
            for j, k in enumerate(ks):
                m = r * n + k
                note_error(row, k, running - olds[j])
                xs[k] = running
                running = running + (wide(coef_one[m]) * olds[j] + wide(coef_two[m]) * noises[j])
            return running

        for i in range(ITERS):
            row = r * ITERS + i
            if n <= GROUP_MOST + 1:
                running = some(row, list(range(i, n - 1)), xs[i])
            else:
                running = lax.fori_loop(i, n - 1, lambda k, held: some(row, [k], held), xs[i])
            note_error(row, n - 1, running - xs[n - 1])
            xs[n - 1] = running
        advance = adv_ref[r]

        def shift(k, carry):
            xs[k] = xs[jnp.minimum(k + advance, n - 1)]
            return carry

        lax.fori_loop(0, n, shift, 0, unroll=4)
        return carry

    lax.fori_loop(0, ROUNDS, one_round, 0)
    for k in range(n):
        fin[k] = xs[k, 0:lat, :]
    each_peer(lambda d: out_copy(d, me).start())
    cells = (ROUNDS * ITERS, LANES)
    diagonal = lax.broadcasted_iota(jnp.int32, cells, 0) == lax.broadcasted_iota(jnp.int32, cells, 1)
    for k in range(n):
        total = jnp.sum(errs[k], axis=1, keepdims=True)
        elines[k] = jnp.sum(jnp.where(diagonal, total, 0.0), axis=0, keepdims=True)
    each_peer(lambda d: err_copy(d, me).start())
    if direct:
        out_ref[0, :, pl.ds(pl.multiple_of(me * pix, LANES), pix)] = fin[me]
    else:
        out_ref[me] = fin[me]
    erecv[me] = elines[me]
    each_peer(lambda d: err_copy(d, d).wait_recv())
    sums = lax.fori_loop(0, n, lambda k, total: total + erecv[k], jnp.zeros((1, LANES), f32), unroll=4)
    means = jnp.sum(jnp.where(diagonal, sums, 0.0), axis=1, keepdims=True) * (1.0 / (lat * n * pix))
    for r in range(ROUNDS):
        err_ref[r] = means[r * ITERS:(r + 1) * ITERS]
    each_peer(lambda d: out_copy(d, d).wait_recv())
    each_peer(lambda d: in_copy(d, me).wait_send())
    each_peer(lambda d: out_copy(d, me).wait_send())
    each_peer(lambda d: err_copy(d, me).wait_send())


def shards(states, t_sched, advances, in_weight, time_weight, mid_weight, out_weight):
    n = lax.axis_size("steps")
    _, lat, rows = states.shape
    ch = mid_weight.shape[0]
    pix = rows // n
    direct = pix % LANES == 0
    width = round_up(pix, LANES)
    depth = round_up(XROWS + 3 * ROUNDS * n, LANES)
    if direct:
        sent = states
        out_shape = states.shape
    else:
        sent = jnp.pad(states.reshape(lat, n, pix).transpose(1, 0, 2), ((0, 0), (0, 0), (0, width - pix)))
        out_shape = sent.shape
    vmem = pl.BlockSpec(memory_space=pltpu.VMEM)
    smem = pl.BlockSpec(memory_space=pltpu.SMEM)
    hbm = pl.BlockSpec(memory_space=pltpu.HBM)
    f32, bf16 = jnp.float32, jnp.bfloat16
    final, errors = pl.pallas_call(
        functools.partial(kernel, n, pix, width, depth, direct),
        out_shape=(jax.ShapeDtypeStruct(out_shape, f32), jax.ShapeDtypeStruct((ROUNDS, ITERS, 1), f32)),
        in_specs=[hbm, smem, smem, smem, hbm, hbm, hbm, hbm, hbm],
        out_specs=(vmem, vmem),
        scratch_shapes=[
            pltpu.VMEM(sent.shape, f32),
            pltpu.VMEM((lat, ch), bf16),
            pltpu.VMEM((lat, ch), bf16),
            pltpu.VMEM((ch, ch), f32),
            pltpu.VMEM((ch, ch), bf16),
            pltpu.VMEM((2 * ch, BASE), f32),
            pltpu.VMEM((n, lat, width), f32),
            pltpu.VMEM((n, 8, width), f32),
            pltpu.VMEM((n, lat, width), f32),
            pltpu.VMEM((n, ROUNDS * ITERS, LANES), f32),
            pltpu.VMEM((n, 1, LANES), f32),
            pltpu.VMEM((n, 1, LANES), f32),
            pltpu.VMEM((ch + 32, depth), bf16),
            pltpu.VMEM((ch, ch), bf16),
            pltpu.VMEM((8, ch), f32),
            pltpu.VMEM((8, ch), f32),
            pltpu.VMEM((ROUNDS * n, 8, LANES), f32),
            pltpu.VMEM((ROUNDS * n, 8, LANES), f32),
            pltpu.SemaphoreType.DMA((6,)),
        ] + [pltpu.SemaphoreType.DMA((n,))] * 6,
        compiler_params=pltpu.CompilerParams(
            collective_id=0, has_side_effects=True, vmem_limit_bytes=67043328),
        name="picard",
    )(sent, t_sched, advances, jnp.asarray(alpha_table()), in_weight.T, out_weight, time_weight, mid_weight,
      jnp.asarray(trig_tables(time_weight.shape[1])))
    if not direct:
        final = final[:, :, :pix].transpose(1, 0, 2).reshape(states.shape)
    return final, errors


def solution(mesh):
    in_specs = (P(("groups", "steps"), None, None), P("groups"), P("groups"), P(), P(), P(), P())
    out_specs = (P(("groups", "steps"), None, None), P("groups", None, "steps"))
    return jax.shard_map(shards, mesh=mesh, in_specs=in_specs, out_specs=out_specs, check_vma=False)
```
